512 devices in a mesh: parts: 2 (over y), shot: 32 (over z), freq: 4 (over x), rep: 2 (over core).
Axes of the slice: x: 4, y: 2, z: 32, core: 2. Of those that a mesh axis runs over, the one named last changes fastest.
The devices are a block of a 4x8x32 slice.
Arguments:
- recorded: bfloat16 [2, 8, 2048, 2048], P(None, ('parts', 'freq'), ('shot', 'rep')), parts along dimension 1, may hold values from -6 to 6
- receiver_x: float32 [4096], P('parts'), parts along dimension 0, may hold values from -12800 to 12800
- source_x: float32 [4096], P('parts'), parts along dimension 0, may hold values from -12800 to 12800
Outputs:
- predicted: bfloat16 [2, 8, 2048, 2048], P(None, ('parts', 'freq'), ('shot', 'rep')), parts along dimension 1
The draws below stay inside these ranges and needn't reach their ends.
There are 2 independent parts, one for each index of `parts`. The reference program is written for one: setup_inputs(seed, part) draws one part's arguments, and reference() takes and returns one part's arrays. A program takes and returns all parts, laid end to end along the dimension named above; each array names one. Nothing has to cross between parts.
All inputs are finite; a program needn't handle non-finite values.
Results may differ from the reference program's by a relative error of at most 0.013.
Values may be sent and summed in bfloat16 or wider, within the bound.
No kernel may reach another device: no remote copies, remote signals or barrier semaphores. Data moves between devices by JAX's collectives and lax.ppermute only.
A program may use at most 64 MiB of HBM per device.

```python
import math
import jax
import jax.numpy as jnp
from jax import lax

NSRC = 2048
NREC = 2048
NSLOW = 1024
NFREQ = 4


def level_of(stream_key, extent, split, least, high):
    gain, own = 1.0, jax.random.fold_in(stream_key, 6)
    for dim, parts in split:
        heights = jnp.exp(jax.random.uniform(jax.random.fold_in(own, dim), (parts,), jnp.float32, least / len(split), high / len(split)))
        gain = gain * jnp.repeat(heights, extent[dim] // parts).reshape([-1 if axis == dim else 1 for axis in range(len(extent))])
    return gain


def scatter_about(own_key, shape, width, limit, shards=(), kind=jnp.bfloat16):
    values = width * jax.random.normal(own_key, shape, jnp.float32)
    if shards:
        values = values * level_of(own_key, shape, shards, -0.22, 0.18)
    return jnp.clip(values, -limit, limit).astype(kind)


def setup_inputs(seed: int = 0, part: int = 0) -> dict:
    keys = jax.random.split(jax.random.key(seed), 4)
    part_keys = jax.random.split(jax.random.fold_in(keys[3], part), 4)
    return {
        "recorded": scatter_about(part_keys[0], (2, NFREQ, NSRC, NREC), 1.0, 6.0, ((1, 4), (2, 64))),
        "receiver_x": jnp.clip(jax.random.uniform(part_keys[1], (NREC,), jnp.float32, -12800.0, 12800.0), -12800.0, 12800.0),
        "source_x": jnp.clip(jax.random.uniform(part_keys[2], (NSRC,), jnp.float32, -12800.0, 12800.0), -12800.0, 12800.0),
    }


two_pi = 6.283185307179586
base_hertz = 40.0
step_hertz = 0.5
slow_max = 0.0005

def slowness_values(grid_count):
    counts = jnp.arange(grid_count, dtype=jnp.int32)
    return slow_max * ((2 * counts + 1 - grid_count).astype(jnp.float32) / grid_count)

def angle_tables(omegas, positions, slowness_grid):
    phases = (omegas * slowness_grid)[None, :] * positions[:, None]
    return (jnp.cos(phases).astype(jnp.bfloat16), jnp.sin(phases).astype(jnp.bfloat16))

def product(left, right):
    return jnp.dot(left, right, preferred_element_type=jnp.float32)

def reference(recorded, receiver_x, source_x):
    slowness_grid = slowness_values(NSLOW)
    scale_receivers = 1.0 / math.sqrt(NREC)
    scale_sources = 1.0 / math.sqrt(NSRC)
    scale_slices = 1.0 / math.sqrt(NSLOW)

    def one_frequency(inputs):
        index_value, data_real, data_imaginary = inputs
        omegas = two_pi * (base_hertz + step_hertz * index_value)
        receiver_cosine, receiver_sine = angle_tables(omegas, receiver_x, slowness_grid)
        source_cosine, source_sine = angle_tables(omegas, source_x, slowness_grid)
        spread_real = ((product(data_real, receiver_cosine) + product(data_imaginary, receiver_sine)) * scale_receivers).astype(jnp.bfloat16)
        spread_imaginary = ((product(data_imaginary, receiver_cosine) - product(data_real, receiver_sine)) * scale_receivers).astype(jnp.bfloat16)
        plane_real = ((product(source_cosine.T, spread_real) + product(source_sine.T, spread_imaginary)) * scale_sources).astype(jnp.bfloat16)
        plane_imaginary = ((product(source_cosine.T, spread_imaginary) - product(source_sine.T, spread_real)) * scale_sources).astype(jnp.bfloat16)
        multiple_real = ((product(plane_real, plane_real) - product(plane_imaginary, plane_imaginary)) * scale_slices).astype(jnp.bfloat16)
        multiple_imaginary = ((product(plane_real, plane_imaginary) + product(plane_imaginary, plane_real)) * scale_slices).astype(jnp.bfloat16)
        back_real = ((product(source_cosine, multiple_real) - product(source_sine, multiple_imaginary)) * scale_slices).astype(jnp.bfloat16)
        back_imaginary = ((product(source_cosine, multiple_imaginary) + product(source_sine, multiple_real)) * scale_slices).astype(jnp.bfloat16)
        predicted_real = ((product(back_real, receiver_cosine.T) - product(back_imaginary, receiver_sine.T)) * scale_slices).astype(jnp.bfloat16)
        predicted_imaginary = ((product(back_real, receiver_sine.T) + product(back_imaginary, receiver_cosine.T)) * scale_slices).astype(jnp.bfloat16)
        return (predicted_real, predicted_imaginary)
    indices = jnp.arange(NFREQ, dtype=jnp.int32).astype(jnp.float32)
    result_real, result_imaginary = lax.map(one_frequency, (indices, recorded[0], recorded[1]))
    return jnp.stack([result_real, result_imaginary], axis=0)
```

```python
import math

import jax
import jax.numpy as jnp
from jax import lax
from jax.experimental import pallas as pl
from jax.experimental.pallas import tpu as pltpu
from jax.sharding import Mesh
from jax.sharding import PartitionSpec as P

NSLOW = 1024
FINE = 8
NEAR = 4

two_pi = 6.283185307179586
base_hertz = 40.0
step_hertz = 0.5
slow_max = 0.0005

GROUP = ("far", "near", "rep")


def source_row(a, b):
    return (b * FINE + a) * 2 * FINE


def receiver_row(a, b):
    half = FINE // 2
    return ((a // half * FINE + b) * half + a % half) * 2 * FINE


def seed_slowness():
    rows = jnp.arange(3 * FINE, dtype=jnp.int32)
    level, index = rows // FINE, rows % FINE
    odd = jnp.where(level == 0, 2 * index + 1, jnp.where(level == 1, 2 * FINE * index, 2 * FINE * FINE * index))
    return slow_max * (odd.astype(jnp.float32) / NSLOW)


def seeds(omega, positions):
    phases = (omega * seed_slowness())[:, None] * positions[None, :]
    return jnp.cos(phases), jnp.sin(phases)


def fill_table(cos_ref, sin_ref, table_ref, row_of):
    width = min(256, table_ref.shape[1])

    def fill(step, carry):
        lanes = pl.ds(pl.multiple_of(step * width, width), width)
        c0, s0 = cos_ref[0:FINE, lanes], sin_ref[0:FINE, lanes]
        inner = [(c0, s0)]
        for b in range(1, FINE):
            cb, sb = cos_ref[pl.ds(FINE + b, 1), lanes], sin_ref[pl.ds(FINE + b, 1), lanes]
            inner.append((c0 * cb - s0 * sb, s0 * cb + c0 * sb))
        for a in range(FINE):
            ca, sa = cos_ref[pl.ds(2 * FINE + a, 1), lanes], sin_ref[pl.ds(2 * FINE + a, 1), lanes]
            for b, (c, s) in enumerate(inner):
                if a > 0:
                    c, s = c * ca - s * sa, s * ca + c * sa
                rows = jnp.concatenate([c, s], axis=0).astype(jnp.bfloat16)
                table_ref[pl.ds(row_of(a, b), 2 * FINE), lanes] = rows
        return carry

    lax.fori_loop(0, table_ref.shape[1] // width, fill, 0)


def dot_last(left, right):
    return lax.dot_general(left, right, (((1,), (1,)), ((), ())), preferred_element_type=jnp.float32)


def split_parts(x, scale):
    lanes = x.shape[1]
    x = (x * scale).reshape(2 * FINE, 2, FINE, lanes)
    return [x[:, part].reshape(2 * FINE * FINE, lanes) for part in range(2)]


def forward_kernel(data_ref, cos_ref, sin_ref, spread_ref, table_ref):
    fill_table(cos_ref, sin_ref, table_ref, receiver_row)
    total = dot_last(table_ref[...], data_ref[...]) * (1.0 / math.sqrt(data_ref.shape[1]))
    for a in range(FINE):
        for b in range(FINE):
            row = receiver_row(a, b)
            pair = [total[row : row + FINE], total[row + FINE : row + 2 * FINE]]
            spread_ref[a * FINE + b] = jnp.concatenate(pair, axis=1).astype(jnp.bfloat16)


def planes_kernel(gathered_ref, cos_ref, sin_ref, planes_ref, table_ref):
    peers, _, lanes = gathered_ref.shape
    shots = table_ref.shape[1] // peers
    fill_table(cos_ref, sin_ref, table_ref, source_row)
    got = gathered_ref[...].astype(jnp.float32)
    lines = []
    for kind in range(lanes // shots):
        pieces = [got[d, :, kind * shots : (kind + 1) * shots] for d in range(peers)]
        lines.append(jnp.concatenate(pieces, axis=1))
    stacked = jnp.concatenate(lines, axis=0).astype(jnp.bfloat16)
    total = dot_last(table_ref[...], stacked) * (1.0 / math.sqrt(table_ref.shape[1]))
    planes_ref[...] = total.T.astype(jnp.bfloat16)


def inner_kernel(planes_ref, cos_ref, sin_ref, inner_ref, table_ref):
    fill_table(cos_ref, sin_ref, table_ref, source_row)
    total = jnp.dot(planes_ref[...], table_ref[...], preferred_element_type=jnp.float32)
    both = jnp.concatenate(split_parts(total, 2.0 / math.sqrt(NSLOW)), axis=1)
    rows = lax.broadcasted_iota(jnp.int32, both.shape, 0)
    inner_ref[...] = jnp.where(rows // FINE % 2 == 0, both, -both).astype(jnp.bfloat16)


def back_kernel(rep_ref, planes_ref, mine_ref, other_ref, back_ref, inner_ref):
    rep = rep_ref[0]
    rows = 2 * FINE * FINE
    for near in range(NEAR):
        first = pl.multiple_of((2 * near + rep) * rows, rows)
        second = pl.multiple_of((2 * near + 1 - rep) * rows, rows)
        inner_ref[pl.ds(first, rows), :] = mine_ref[near * rows : (near + 1) * rows, :]
        inner_ref[pl.ds(second, rows), :] = other_ref[near * rows : (near + 1) * rows, :]
    total = jnp.dot(planes_ref[...], inner_ref[...], preferred_element_type=jnp.float32)
    upper, lower = split_parts(total, 2.0 / math.sqrt(NSLOW))
    shots = upper.shape[1] // 2
    real = upper[:, :shots] - lower[:, shots:]
    imaginary = lower[:, :shots] + upper[:, shots:]
    peers, half, lanes = back_ref.shape
    own = lanes // 4
    for peer in range(peers):
        span = slice(peer * own, (peer + 1) * own)
        pieces = [real[:half, span], imaginary[:half, span], real[half:, span], imaginary[half:, span]]
        back_ref[peer] = jnp.concatenate(pieces, axis=1).astype(jnp.bfloat16)


def inverse_kernel(back_ref, cos_ref, sin_ref, out_ref, table_ref):
    fill_table(cos_ref, sin_ref, table_ref, receiver_row)
    peers, half, lanes = back_ref.shape
    turned = back_ref[...].astype(jnp.float32).reshape(peers * half, lanes).T
    back = jnp.concatenate([turned[: lanes // 2], turned[lanes // 2 :]], axis=1).astype(jnp.bfloat16)
    total = jnp.dot(back, table_ref[...], preferred_element_type=jnp.float32)
    out_ref[...] = (total * (2.0 / math.sqrt(NSLOW))).astype(jnp.bfloat16)


def call(kernel, shape, scratch, *operands):
    spec = pl.BlockSpec(memory_space=pltpu.VMEM)
    scalar = pl.BlockSpec(memory_space=pltpu.SMEM)
    return pl.pallas_call(
        kernel,
        out_shape=jax.ShapeDtypeStruct(shape, jnp.bfloat16),
        in_specs=[scalar if x.dtype == jnp.int32 else spec for x in operands],
        out_specs=spec,
        scratch_shapes=[pltpu.VMEM(scratch, jnp.bfloat16)],
        compiler_params=pltpu.CompilerParams(vmem_limit_bytes=40 * 2**20),
    )(*operands)


def body(recorded, receiver_x, source_x):
    _, _, shots, receivers = recorded.shape
    sources = source_x.shape[0]
    near_peers = lax.axis_size("near") * lax.axis_size("rep")
    peers = lax.axis_size("far") * near_peers
    far, rep = lax.axis_index("far"), lax.axis_index("rep")
    omega = two_pi * (base_hertz + step_hertz * lax.axis_index("freq").astype(jnp.float32))
    data = recorded.reshape(2 * shots, receivers)

    receiver_seeds = seeds(omega, receiver_x)
    spread = call(forward_kernel, (peers, FINE, 4 * shots), (NSLOW, receivers), data, *receiver_seeds)
    gathered = lax.all_to_all(spread, GROUP, 0, 0, tiled=True)

    source_seeds = seeds(omega, source_x)
    planes = call(planes_kernel, (4 * FINE, NSLOW), (NSLOW, sources), gathered, *source_seeds)
    planes = lax.all_gather(planes, "far", axis=0, tiled=True)

    around = near_peers * shots
    around_seeds = [lax.dynamic_slice_in_dim(x, far * around, around, 1) for x in source_seeds]
    inner = call(inner_kernel, (2 * FINE * FINE, 2 * around), (NSLOW, around), planes, *around_seeds)
    mine = lax.all_gather(inner, "near", axis=0, tiled=True)
    other = lax.ppermute(mine, "rep", [(0, 1), (1, 0)])
    back = call(
        back_kernel,
        (near_peers, FINE * FINE, 4 * shots),
        (NSLOW, 2 * around),
        rep.astype(jnp.int32).reshape(1),
        planes,
        mine,
        other,
    )
    back = lax.all_to_all(back, ("near", "rep"), 0, 0, tiled=True)
    out = call(inverse_kernel, (2 * shots, receivers), (NSLOW, receivers), back, *receiver_seeds)
    return out.reshape(recorded.shape)


def solution(mesh):
    parts, shot, freq, rep = (mesh.shape[name] for name in ("parts", "shot", "freq", "rep"))
    devices = mesh.devices.reshape(parts, shot // NEAR, NEAR, freq, rep)
    split = Mesh(devices, ("parts", "far", "near", "freq", "rep"))
    placed = P(None, ("parts", "freq"), GROUP, None)
    return jax.shard_map(
        body,
        mesh=split,
        in_specs=(placed, P("parts"), P("parts")),
        out_specs=placed,
        check_vma=False,
    )
```

```python
import math

import jax
import jax.numpy as jnp
from jax import lax
from jax.experimental import pallas as pl
from jax.experimental.pallas import tpu as pltpu
from jax.sharding import Mesh
from jax.sharding import PartitionSpec as P

NSLOW = 1024
FINE = 8
NEAR = 4

two_pi = 6.283185307179586
base_hertz = 40.0
step_hertz = 0.5
slow_max = 0.0005

GROUP = ("far", "near", "rep")


def source_row(kind, a, b):
    return ((b * 2 + kind) * FINE + a) * FINE


def receiver_row(kind, a, b):
    return ((kind * FINE + b) * FINE + a) * FINE


def seed_slowness():
    rows = jnp.arange(3 * FINE, dtype=jnp.int32)
    level, index = rows // FINE, rows % FINE
    odd = jnp.where(level == 0, 2 * index + 1, jnp.where(level == 1, 2 * FINE * index, 2 * FINE * FINE * index))
    return slow_max * (odd.astype(jnp.float32) / NSLOW)


def seeds(omega, positions):
    phases = (omega * seed_slowness())[:, None] * positions[None, :]
    return jnp.cos(phases), jnp.sin(phases)


def fill_table(cos_ref, sin_ref, table_ref, row_of):
    width = min(256, table_ref.shape[1])

    def fill(step, carry):
        lanes = pl.ds(pl.multiple_of(step * width, width), width)
        c0, s0 = cos_ref[0:FINE, lanes], sin_ref[0:FINE, lanes]
        inner = [(c0, s0)]
        for b in range(1, FINE):
            cb, sb = cos_ref[pl.ds(FINE + b, 1), lanes], sin_ref[pl.ds(FINE + b, 1), lanes]
            inner.append((c0 * cb - s0 * sb, s0 * cb + c0 * sb))
        for a in range(0, FINE, 2):
            turns = [
                (cos_ref[pl.ds(2 * FINE + k, 1), lanes], sin_ref[pl.ds(2 * FINE + k, 1), lanes]) for k in (a, a + 1)
            ]
            for b, (c, s) in enumerate(inner):
                pairs = [(c * ca - s * sa, s * ca + c * sa) for ca, sa in turns]
                for kind in range(2):
                    rows = jnp.concatenate([pair[kind] for pair in pairs], axis=0).astype(jnp.bfloat16)
                    table_ref[pl.ds(row_of(kind, a, b), 2 * FINE), lanes] = rows
        return carry

    lax.fori_loop(0, table_ref.shape[1] // width, fill, 0)


def dot_last(left, right):
    return lax.dot_general(left, right, (((1,), (1,)), ((), ())), preferred_element_type=jnp.float32)


def split_parts(x, scale):
    rows, lanes = x.shape
    x = (x * scale).reshape(2, 2, rows // 4, lanes)
    return [x[:, part].reshape(rows // 2, lanes) for part in range(2)]


def forward_kernel(data_ref, cos_ref, sin_ref, spread_ref, table_ref):
    fill_table(cos_ref, sin_ref, table_ref, receiver_row)
    total = dot_last(table_ref[...], data_ref[...]) * (1.0 / math.sqrt(data_ref.shape[1]))
    half = total.shape[0] // 2
    both = jnp.concatenate([total[:half], total[half:]], axis=1)
    spread_ref[...] = both.reshape(spread_ref.shape).astype(jnp.bfloat16)


def turn_kernel(near_ref, main_ref, rest_ref):
    peers, rows, lanes = near_ref.shape
    shots = lanes // 4
    got = near_ref[...].astype(jnp.float32)
    lines = []
    for kind in range(4):
        pieces = [got[d, :, kind * shots : (kind + 1) * shots] for d in range(peers)]
        lines.append(jnp.concatenate(pieces, axis=1))
    turned = jnp.concatenate(lines, axis=0).astype(jnp.bfloat16)
    main = main_ref.shape[0]
    main_ref[...] = turned[:main]
    for far in range(rest_ref.shape[0]):
        rest_ref[far] = turned[main:]


def planes_kernel(far_ref, main_ref, rest_ref, cos_ref, sin_ref, planes_ref, inner_ref, table_ref, spread_ref):
    fill_table(cos_ref, sin_ref, table_ref, source_row)
    peers, main, around = main_ref.shape
    for far in range(peers):
        spread_ref[:main, far * around : (far + 1) * around] = main_ref[far]
        spread_ref[main:, far * around : (far + 1) * around] = rest_ref[far]
    total = dot_last(table_ref[...], spread_ref[...]) * (1.0 / math.sqrt(table_ref.shape[1]))
    planes = total.T.astype(jnp.bfloat16)
    planes_ref[...] = planes
    own = table_ref[:, pl.ds(pl.multiple_of(far_ref[0] * around, around), around)]
    total = jnp.dot(planes, own, preferred_element_type=jnp.float32)
    both = jnp.concatenate(split_parts(total, 2.0 / math.sqrt(NSLOW)), axis=1)
    half = both.shape[0] // 2
    inner_ref[:half] = both[:half].astype(jnp.bfloat16)
    inner_ref[half:] = (-both[half:]).astype(jnp.bfloat16)


def back_kernel(rep_ref, planes_ref, mine_ref, other_ref, back_ref, inner_ref):
    rep = rep_ref[0]
    rows = 2 * FINE * FINE
    for near in range(NEAR):
        first = pl.multiple_of((2 * near + rep) * rows, rows)
        second = pl.multiple_of((2 * near + 1 - rep) * rows, rows)
        inner_ref[pl.ds(first, rows), :] = mine_ref[near * rows : (near + 1) * rows, :]
        inner_ref[pl.ds(second, rows), :] = other_ref[near * rows : (near + 1) * rows, :]
    total = jnp.dot(planes_ref[...], inner_ref[...], preferred_element_type=jnp.float32)
    upper, lower = split_parts(total, 2.0 / math.sqrt(NSLOW))
    shots = upper.shape[1] // 2
    real = upper[:, :shots] - lower[:, shots:]
    imaginary = lower[:, :shots] + upper[:, shots:]
    peers, half, lanes = back_ref.shape
    own = lanes // 4
    for peer in range(peers):
        span = slice(peer * own, (peer + 1) * own)
        pieces = [real[:half, span], imaginary[:half, span], real[half:, span], imaginary[half:, span]]
        back_ref[peer] = jnp.concatenate(pieces, axis=1).astype(jnp.bfloat16)


def inverse_kernel(back_ref, cos_ref, sin_ref, out_ref, table_ref):
    fill_table(cos_ref, sin_ref, table_ref, receiver_row)
    peers, half, lanes = back_ref.shape
    turned = back_ref[...].astype(jnp.float32).reshape(peers * half, lanes).T
    back = jnp.concatenate([turned[: lanes // 2], turned[lanes // 2 :]], axis=1).astype(jnp.bfloat16)
    total = jnp.dot(back, table_ref[...], preferred_element_type=jnp.float32)
    out_ref[...] = (total * (2.0 / math.sqrt(NSLOW))).astype(jnp.bfloat16)


def call(kernel, shapes, scratch, *operands):
    spec = pl.BlockSpec(memory_space=pltpu.VMEM)
    scalar = pl.BlockSpec(memory_space=pltpu.SMEM)
    return pl.pallas_call(
        kernel,
        out_shape=[jax.ShapeDtypeStruct(shape, jnp.bfloat16) for shape in shapes],
        in_specs=[scalar if x.dtype == jnp.int32 else spec for x in operands],
        out_specs=[spec] * len(shapes),
        scratch_shapes=[pltpu.VMEM(shape, jnp.bfloat16) for shape in scratch],
        compiler_params=pltpu.CompilerParams(vmem_limit_bytes=40 * 2**20),
    )(*operands)


def body(recorded, receiver_x, source_x):
    _, _, shots, receivers = recorded.shape
    sources = source_x.shape[0]
    near = ("near", "rep")
    peers = lax.axis_size("near") * lax.axis_size("rep")
    around = peers * shots
    far_peers = lax.axis_size("far")
    far, rep = [lax.axis_index(name).astype(jnp.int32).reshape(1) for name in ("far", "rep")]
    omega = two_pi * (base_hertz + step_hertz * lax.axis_index("freq").astype(jnp.float32))
    data = recorded.reshape(2 * shots, receivers)
    receiver_seeds = seeds(omega, receiver_x)
    source_seeds = seeds(omega, source_x)
    receiver_table, source_table = (NSLOW, receivers), (NSLOW, sources)
    columns = 2 * NSLOW // peers
    rest = columns // 16
    chunk = (peers, FINE * FINE, 4 * shots)

    (spread,) = call(forward_kernel, [chunk], [receiver_table], data, *receiver_seeds)
    spread = lax.all_to_all(spread, near, 0, 0, tiled=True)
    most, last = call(turn_kernel, [(columns - rest, around), (far_peers, rest, around)], [], spread)
    last = lax.all_to_all(last, "far", 0, 0, tiled=True)
    most = lax.all_gather(most, "far", axis=0, tiled=False)
    planes, inner = call(
        planes_kernel,
        [(columns, NSLOW), (columns // 2, 2 * around)],
        [source_table, (columns, sources)],
        far,
        most,
        last,
        *source_seeds,
    )
    mine = lax.all_gather(inner, "near", axis=0, tiled=True)
    other = lax.ppermute(mine, "rep", [(0, 1), (1, 0)])
    (back,) = call(back_kernel, [chunk], [(NSLOW, 2 * around)], rep, planes, mine, other)
    back = lax.all_to_all(back, near, 0, 0, tiled=True)
    (out,) = call(inverse_kernel, [(2 * shots, receivers)], [receiver_table], back, *receiver_seeds)
    return out.reshape(recorded.shape)


def solution(mesh):
    parts, shot, freq, rep = (mesh.shape[name] for name in ("parts", "shot", "freq", "rep"))
    devices = mesh.devices.reshape(parts, shot // NEAR, NEAR, freq, rep)
    split = Mesh(devices, ("parts", "far", "near", "freq", "rep"))
    placed = P(None, ("parts", "freq"), GROUP, None)
    return jax.shard_map(
        body,
        mesh=split,
        in_specs=(placed, P("parts"), P("parts")),
        out_specs=placed,
        check_vma=False,
    )
```

```python
import math

import jax
import jax.numpy as jnp
from jax import lax
from jax.experimental import pallas as pl
from jax.experimental.pallas import tpu as pltpu
from jax.sharding import Mesh
from jax.sharding import PartitionSpec as P

NSLOW = 1024
FINE = 8
NEAR = 4

two_pi = 6.283185307179586
base_hertz = 40.0
step_hertz = 0.5
slow_max = 0.0005

GROUP = ("far", "near", "rep")


def source_row(kind, a, b):
    return ((b * 2 + kind) * FINE + a) * FINE


def receiver_row(kind, a, b):
    return ((kind * FINE + b) * FINE + a) * FINE


def seed_slowness():
    rows = jnp.arange(3 * FINE, dtype=jnp.int32)
    level, index = rows // FINE, rows % FINE
    odd = jnp.where(level == 0, 2 * index + 1, jnp.where(level == 1, 2 * FINE * index, 2 * FINE * FINE * index))
    return slow_max * (odd.astype(jnp.float32) / NSLOW)


def seeds(omega, positions):
    phases = (omega * seed_slowness())[:, None] * positions[None, :]
    return jnp.cos(phases), jnp.sin(phases)


def fill_table(cos_ref, sin_ref, table_ref, row_of):
    width = min(256, table_ref.shape[1])

    def fill(step, carry):
        lanes = pl.ds(pl.multiple_of(step * width, width), width)
        c0, s0 = cos_ref[0:FINE, lanes], sin_ref[0:FINE, lanes]
        inner = [(c0, s0)]
        for b in range(1, FINE):
            cb, sb = cos_ref[pl.ds(FINE + b, 1), lanes], sin_ref[pl.ds(FINE + b, 1), lanes]
            inner.append((c0 * cb - s0 * sb, s0 * cb + c0 * sb))
        for a in range(0, FINE, 2):
            turns = [
                (cos_ref[pl.ds(2 * FINE + k, 1), lanes], sin_ref[pl.ds(2 * FINE + k, 1), lanes]) for k in (a, a + 1)
            ]
            for b, (c, s) in enumerate(inner):
                pairs = [(c * ca - s * sa, s * ca + c * sa) for ca, sa in turns]
                for kind in range(2):
                    rows = jnp.concatenate([pair[kind] for pair in pairs], axis=0).astype(jnp.bfloat16)
                    table_ref[pl.ds(row_of(kind, a, b), 2 * FINE), lanes] = rows
        return carry

    lax.fori_loop(0, table_ref.shape[1] // width, fill, 0)


def dot_last(left, right):
    return lax.dot_general(left, right, (((1,), (1,)), ((), ())), preferred_element_type=jnp.float32)


def split_parts(x, scale):
    rows, lanes = x.shape
    x = (x * scale).reshape(2, 2, rows // 4, lanes)
    return [x[:, part].reshape(rows // 2, lanes) for part in range(2)]


def forward_kernel(data_ref, cos_ref, sin_ref, spread_ref, table_ref):
    fill_table(cos_ref, sin_ref, table_ref, receiver_row)
    total = dot_last(table_ref[...], data_ref[...]) * (1.0 / math.sqrt(data_ref.shape[1]))
    half = total.shape[0] // 2
    both = jnp.concatenate([total[:half], total[half:]], axis=1)
    spread_ref[...] = both.reshape(spread_ref.shape).astype(jnp.bfloat16)


LEVEL = 13.0
LEAST = 2.0**-100


def turn_kernel(near_ref, turned_ref):
    peers, rows, lanes = near_ref.shape
    shots = lanes // 4
    got = near_ref[...].astype(jnp.float32)
    lines = []
    for kind in range(4):
        pieces = [got[d, :, kind * shots : (kind + 1) * shots] for d in range(peers)]
        lines.append(jnp.concatenate(pieces, axis=1))
    turned = jnp.concatenate(lines, axis=0)
    largest = jnp.maximum(jnp.max(jnp.abs(turned), keepdims=True), LEAST)
    exponent = jnp.ceil(jnp.log2(largest))
    main = 4 * rows
    turned_ref[:main] = (turned * jnp.exp2(LEVEL - exponent)).astype(turned_ref.dtype)
    tail = jnp.broadcast_to(exponent, (turned_ref.shape[0] - main, turned.shape[1]))
    turned_ref[main:] = tail.astype(turned_ref.dtype)


def planes_kernel(far_ref, turned_ref, cos_ref, sin_ref, planes_ref, inner_ref, table_ref, spread_ref):
    fill_table(cos_ref, sin_ref, table_ref, source_row)
    peers, _, around = turned_ref.shape
    main = spread_ref.shape[0]
    for far in range(peers):
        block = turned_ref[far].astype(jnp.float32)
        block = block[:main] * jnp.exp2(block[main : main + 1, :1] - LEVEL)
        spread_ref[:, far * around : (far + 1) * around] = block.astype(jnp.bfloat16)
    total = dot_last(table_ref[...], spread_ref[...]) * (1.0 / math.sqrt(table_ref.shape[1]))
    planes = total.T.astype(jnp.bfloat16)
    planes_ref[...] = planes
    own = table_ref[:, pl.ds(pl.multiple_of(far_ref[0] * around, around), around)]
    total = jnp.dot(planes, own, preferred_element_type=jnp.float32)
    both = jnp.concatenate(split_parts(total, 2.0 / math.sqrt(NSLOW)), axis=1)
    half = both.shape[0] // 2
    inner_ref[:half] = both[:half].astype(jnp.bfloat16)
    inner_ref[half:] = (-both[half:]).astype(jnp.bfloat16)


def back_kernel(rep_ref, planes_ref, mine_ref, other_ref, back_ref, inner_ref):
    rep = rep_ref[0]
    rows = 2 * FINE * FINE
    for near in range(NEAR):
        first = pl.multiple_of((2 * near + rep) * rows, rows)
        second = pl.multiple_of((2 * near + 1 - rep) * rows, rows)
        inner_ref[pl.ds(first, rows), :] = mine_ref[near * rows : (near + 1) * rows, :]
        inner_ref[pl.ds(second, rows), :] = other_ref[near * rows : (near + 1) * rows, :]
    total = jnp.dot(planes_ref[...], inner_ref[...], preferred_element_type=jnp.float32)
    upper, lower = split_parts(total, 2.0 / math.sqrt(NSLOW))
    shots = upper.shape[1] // 2
    real = upper[:, :shots] - lower[:, shots:]
    imaginary = lower[:, :shots] + upper[:, shots:]
    peers, half, lanes = back_ref.shape
    own = lanes // 4
    for peer in range(peers):
        span = slice(peer * own, (peer + 1) * own)
        pieces = [real[:half, span], imaginary[:half, span], real[half:, span], imaginary[half:, span]]
        back_ref[peer] = jnp.concatenate(pieces, axis=1).astype(jnp.bfloat16)


def inverse_kernel(back_ref, cos_ref, sin_ref, out_ref, table_ref):
    fill_table(cos_ref, sin_ref, table_ref, receiver_row)
    peers, half, lanes = back_ref.shape
    turned = back_ref[...].astype(jnp.float32).reshape(peers * half, lanes).T
    back = jnp.concatenate([turned[: lanes // 2], turned[lanes // 2 :]], axis=1).astype(jnp.bfloat16)
    total = jnp.dot(back, table_ref[...], preferred_element_type=jnp.float32)
    out_ref[...] = (total * (2.0 / math.sqrt(NSLOW))).astype(jnp.bfloat16)


def call(kernel, shapes, scratch, *operands, dtype=jnp.bfloat16):
    spec = pl.BlockSpec(memory_space=pltpu.VMEM)
    scalar = pl.BlockSpec(memory_space=pltpu.SMEM)
    return pl.pallas_call(
        kernel,
        out_shape=[jax.ShapeDtypeStruct(shape, dtype) for shape in shapes],
        in_specs=[scalar if x.dtype == jnp.int32 else spec for x in operands],
        out_specs=[spec] * len(shapes),
        scratch_shapes=[pltpu.VMEM(shape, jnp.bfloat16) for shape in scratch],
        compiler_params=pltpu.CompilerParams(vmem_limit_bytes=40 * 2**20),
    )(*operands)


def body(recorded, receiver_x, source_x):
    _, _, shots, receivers = recorded.shape
    sources = source_x.shape[0]
    near = ("near", "rep")
    peers = lax.axis_size("near") * lax.axis_size("rep")
    around = peers * shots
    far, rep = [lax.axis_index(name).astype(jnp.int32).reshape(1) for name in ("far", "rep")]
    omega = two_pi * (base_hertz + step_hertz * lax.axis_index("freq").astype(jnp.float32))
    data = recorded.reshape(2 * shots, receivers)
    receiver_seeds = seeds(omega, receiver_x)
    source_seeds = seeds(omega, source_x)
    receiver_table, source_table = (NSLOW, receivers), (NSLOW, sources)
    columns = 2 * NSLOW // peers
    chunk = (peers, FINE * FINE, 4 * shots)

    (spread,) = call(forward_kernel, [chunk], [receiver_table], data, *receiver_seeds)
    spread = lax.all_to_all(spread, near, 0, 0, tiled=True)
    (turned,) = call(turn_kernel, [(columns + FINE, around)], [], spread, dtype=jnp.float32)
    turned = lax.all_gather(turned.astype(jnp.float16), "far", axis=0, tiled=False).astype(jnp.float32)
    planes, inner = call(
        planes_kernel,
        [(columns, NSLOW), (columns // 2, 2 * around)],
        [source_table, (columns, sources)],
        far,
        turned,
        *source_seeds,
    )
    mine = lax.all_gather(inner, "near", axis=0, tiled=True)
    other = lax.ppermute(mine, "rep", [(0, 1), (1, 0)])
    (back,) = call(back_kernel, [chunk], [(NSLOW, 2 * around)], rep, planes, mine, other)
    back = lax.all_to_all(back, near, 0, 0, tiled=True)
    (out,) = call(inverse_kernel, [(2 * shots, receivers)], [receiver_table], back, *receiver_seeds)
    return out.reshape(recorded.shape)


def solution(mesh):
    parts, shot, freq, rep = (mesh.shape[name] for name in ("parts", "shot", "freq", "rep"))
    devices = mesh.devices.reshape(parts, shot // NEAR, NEAR, freq, rep)
    split = Mesh(devices, ("parts", "far", "near", "freq", "rep"))
    placed = P(None, ("parts", "freq"), GROUP, None)
    return jax.shard_map(
        body,
        mesh=split,
        in_specs=(placed, P("parts"), P("parts")),
        out_specs=placed,
        check_vma=False,
    )
```

```python
import math

import jax
import jax.numpy as jnp
from jax import lax
from jax.experimental import pallas as pl
from jax.experimental.pallas import tpu as pltpu
from jax.sharding import Mesh
from jax.sharding import PartitionSpec as P

NSLOW = 1024
FINE = 8
NEAR = 2
OWNED = 2

two_pi = 6.283185307179586
base_hertz = 40.0
step_hertz = 0.5
slow_max = 0.0005

GROUP = ("far", "near", "rep")


def source_row(kind, a, b):
    return (((b // OWNED * 2 + kind) * OWNED + b % OWNED) * FINE + a) * FINE


def receiver_row(kind, a, b):
    return ((kind * FINE + b) * FINE + a) * FINE


def seed_slowness():
    rows = jnp.arange(3 * FINE, dtype=jnp.int32)
    level, index = rows // FINE, rows % FINE
    odd = jnp.where(level == 0, 2 * index + 1, jnp.where(level == 1, 2 * FINE * index, 2 * FINE * FINE * index))
    return slow_max * (odd.astype(jnp.float32) / NSLOW)


def seeds(omega, positions):
    phases = (omega * seed_slowness())[:, None] * positions[None, :]
    return jnp.cos(phases), jnp.sin(phases)


def fill_table(cos_ref, sin_ref, table_ref, row_of):
    width = min(256, table_ref.shape[1])

    def fill(step, carry):
        lanes = pl.ds(pl.multiple_of(step * width, width), width)
        c0, s0 = cos_ref[0:FINE, lanes], sin_ref[0:FINE, lanes]
        inner = [(c0, s0)]
        for b in range(1, FINE):
            cb, sb = cos_ref[pl.ds(FINE + b, 1), lanes], sin_ref[pl.ds(FINE + b, 1), lanes]
            inner.append((c0 * cb - s0 * sb, s0 * cb + c0 * sb))
        for a in range(0, FINE, 2):
            turns = [
                (cos_ref[pl.ds(2 * FINE + k, 1), lanes], sin_ref[pl.ds(2 * FINE + k, 1), lanes]) for k in (a, a + 1)
            ]
            for b, (c, s) in enumerate(inner):
                pairs = [(c * ca - s * sa, s * ca + c * sa) for ca, sa in turns]
                for kind in range(2):
                    rows = jnp.concatenate([pair[kind] for pair in pairs], axis=0).astype(jnp.bfloat16)
                    table_ref[pl.ds(row_of(kind, a, b), 2 * FINE), lanes] = rows
        return carry

    lax.fori_loop(0, table_ref.shape[1] // width, fill, 0)


def dot_last(left, right):
    return lax.dot_general(left, right, (((1,), (1,)), ((), ())), preferred_element_type=jnp.float32)


def split_parts(x, scale):
    rows, lanes = x.shape
    x = (x * scale).reshape(2, 2, rows // 4, lanes)
    return [x[:, part].reshape(rows // 2, lanes) for part in range(2)]


def forward_kernel(data_ref, cos_ref, sin_ref, spread_ref, table_ref):
    fill_table(cos_ref, sin_ref, table_ref, receiver_row)
    total = dot_last(table_ref[...], data_ref[...]) * (1.0 / math.sqrt(data_ref.shape[1]))
    half = total.shape[0] // 2
    both = jnp.concatenate([total[:half], total[half:]], axis=1)
    spread_ref[...] = both.reshape(spread_ref.shape).astype(jnp.bfloat16)


LEVEL = 13.0
LEAST = 2.0**-100


def turn_kernel(near_ref, turned_ref):
    peers, rows, lanes = near_ref.shape
    shots = lanes // 4
    got = near_ref[...].astype(jnp.float32)
    lines = []
    for kind in range(4):
        pieces = [got[d, :, kind * shots : (kind + 1) * shots] for d in range(peers)]
        lines.append(jnp.concatenate(pieces, axis=1))
    turned = jnp.concatenate(lines, axis=0)
    largest = jnp.maximum(jnp.max(jnp.abs(turned), keepdims=True), LEAST)
    exponent = jnp.ceil(jnp.log2(largest))
    main = 4 * rows
    turned_ref[:main] = (turned * jnp.exp2(LEVEL - exponent)).astype(turned_ref.dtype)
    tail = jnp.broadcast_to(exponent, (turned_ref.shape[0] - main, turned.shape[1]))
    turned_ref[main:] = tail.astype(turned_ref.dtype)


def planes_kernel(far_ref, turned_ref, cos_ref, sin_ref, planes_ref, inner_ref, table_ref, spread_ref):
    fill_table(cos_ref, sin_ref, table_ref, source_row)
    peers, _, around = turned_ref.shape
    main = spread_ref.shape[0]
    for far in range(peers):
        block = turned_ref[far].astype(jnp.float32)
        block = block[:main] * jnp.exp2(block[main : main + 1, :1] - LEVEL)
        spread_ref[:, far * around : (far + 1) * around] = block.astype(jnp.bfloat16)
    total = dot_last(table_ref[...], spread_ref[...]) * (1.0 / math.sqrt(table_ref.shape[1]))
    planes = total.T.astype(jnp.bfloat16)
    planes_ref[...] = planes
    own = table_ref[:, pl.ds(pl.multiple_of(far_ref[0] * around, around), around)]
    total = jnp.dot(planes, own, preferred_element_type=jnp.float32)
    both = jnp.concatenate(split_parts(total, 2.0 / math.sqrt(NSLOW)), axis=1)
    half = both.shape[0] // 2
    inner_ref[:half] = both[:half].astype(jnp.bfloat16)
    inner_ref[half:] = (-both[half:]).astype(jnp.bfloat16)


def back_kernel(planes_ref, inner_ref, back_ref):
    total = jnp.dot(planes_ref[...], inner_ref[...], preferred_element_type=jnp.float32)
    upper, lower = split_parts(total, 2.0 / math.sqrt(NSLOW))
    shots = upper.shape[1] // 2
    real = upper[:, :shots] - lower[:, shots:]
    imaginary = lower[:, :shots] + upper[:, shots:]
    peers, half, lanes = back_ref.shape
    own = lanes // 4
    for peer in range(peers):
        span = slice(peer * own, (peer + 1) * own)
        pieces = [real[:half, span], imaginary[:half, span], real[half:, span], imaginary[half:, span]]
        back_ref[peer] = jnp.concatenate(pieces, axis=1).astype(jnp.bfloat16)


def inverse_kernel(back_ref, cos_ref, sin_ref, out_ref, table_ref):
    fill_table(cos_ref, sin_ref, table_ref, receiver_row)
    peers, half, lanes = back_ref.shape
    turned = back_ref[...].astype(jnp.float32).reshape(peers * half, lanes).T
    back = jnp.concatenate([turned[: lanes // 2], turned[lanes // 2 :]], axis=1).astype(jnp.bfloat16)
    total = jnp.dot(back, table_ref[...], preferred_element_type=jnp.float32)
    out_ref[...] = (total * (2.0 / math.sqrt(NSLOW))).astype(jnp.bfloat16)


def call(kernel, shapes, scratch, *operands, dtype=jnp.bfloat16):
    spec = pl.BlockSpec(memory_space=pltpu.VMEM)
    scalar = pl.BlockSpec(memory_space=pltpu.SMEM)
    return pl.pallas_call(
        kernel,
        out_shape=[jax.ShapeDtypeStruct(shape, dtype) for shape in shapes],
        in_specs=[scalar if x.dtype == jnp.int32 else spec for x in operands],
        out_specs=[spec] * len(shapes),
        scratch_shapes=[pltpu.VMEM(shape, jnp.bfloat16) for shape in scratch],
        compiler_params=pltpu.CompilerParams(vmem_limit_bytes=40 * 2**20),
    )(*operands)


def body(recorded, receiver_x, source_x):
    _, _, shots, receivers = recorded.shape
    sources = source_x.shape[0]
    near = ("near", "rep")
    peers = lax.axis_size("near") * lax.axis_size("rep")
    around = peers * shots
    far = lax.axis_index("far").astype(jnp.int32).reshape(1)
    omega = two_pi * (base_hertz + step_hertz * lax.axis_index("freq").astype(jnp.float32))
    data = recorded.reshape(2 * shots, receivers)
    receiver_seeds = seeds(omega, receiver_x)
    source_seeds = seeds(omega, source_x)
    receiver_table, source_table = (NSLOW, receivers), (NSLOW, sources)
    columns = 2 * NSLOW // peers
    chunk = (peers, OWNED * FINE * FINE, 4 * shots)

    (spread,) = call(forward_kernel, [chunk], [receiver_table], data, *receiver_seeds)
    spread = lax.all_to_all(spread, near, 0, 0, tiled=True)
    (turned,) = call(turn_kernel, [(columns + FINE, around)], [], spread, dtype=jnp.float32)
    turned = lax.all_gather(turned.astype(jnp.float16), "far", axis=0, tiled=False).astype(jnp.float32)
    planes, inner = call(
        planes_kernel,
        [(columns, NSLOW), (columns // 2, 2 * around)],
        [source_table, (columns, sources)],
        far,
        turned,
        *source_seeds,
    )
    inner = lax.all_gather(inner, near, axis=0, tiled=True)
    (back,) = call(back_kernel, [chunk], [], planes, inner)
    back = lax.all_to_all(back, near, 0, 0, tiled=True)
    (out,) = call(inverse_kernel, [(2 * shots, receivers)], [receiver_table], back, *receiver_seeds)
    return out.reshape(recorded.shape)


def solution(mesh):
    parts, shot, freq, rep = (mesh.shape[name] for name in ("parts", "shot", "freq", "rep"))
    devices = mesh.devices.reshape(parts, shot // NEAR, NEAR, freq, rep)
    split = Mesh(devices, ("parts", "far", "near", "freq", "rep"))
    placed = P(None, ("parts", "freq"), GROUP, None)
    return jax.shard_map(
        body,
        mesh=split,
        in_specs=(placed, P("parts"), P("parts")),
        out_specs=placed,
        check_vma=False,
    )
```

```python
import math

import jax
import jax.numpy as jnp
from jax import lax
from jax.experimental import pallas as pl
from jax.experimental.pallas import tpu as pltpu
from jax.sharding import Mesh
from jax.sharding import PartitionSpec as P

NSLOW = 1024
FINE = 8
NEAR = 2
OWNED = 2

two_pi = 6.283185307179586
base_hertz = 40.0
step_hertz = 0.5
slow_max = 0.0005

GROUP = ("far", "near", "rep")


def source_row(kind, a, b):
    return (((b // OWNED * 2 + kind) * OWNED + b % OWNED) * FINE + a) * FINE


def receiver_row(kind, a, b):
    return ((kind * FINE + b) * FINE + a) * FINE


def seed_slowness():
    rows = jnp.arange(3 * FINE, dtype=jnp.int32)
    level, index = rows // FINE, rows % FINE
    odd = jnp.where(level == 0, 2 * index + 1, jnp.where(level == 1, 2 * FINE * index, 2 * FINE * FINE * index))
    return slow_max * (odd.astype(jnp.float32) / NSLOW)


def seeds(omega, positions):
    phases = (omega * seed_slowness())[:, None] * positions[None, :]
    return jnp.cos(phases), jnp.sin(phases)


WIDTH = 256


def fill_lanes(cos_ref, sin_ref, table_ref, row_of, first):
    lanes = pl.ds(first, WIDTH)
    c0, s0 = cos_ref[0:FINE, lanes], sin_ref[0:FINE, lanes]
    inner = [(c0, s0)]
    for b in range(1, FINE):
        cb, sb = cos_ref[pl.ds(FINE + b, 1), lanes], sin_ref[pl.ds(FINE + b, 1), lanes]
        inner.append((c0 * cb - s0 * sb, s0 * cb + c0 * sb))
    for a in range(0, FINE, 2):
        turns = [(cos_ref[pl.ds(2 * FINE + k, 1), lanes], sin_ref[pl.ds(2 * FINE + k, 1), lanes]) for k in (a, a + 1)]
        for b, (c, s) in enumerate(inner):
            pairs = [(c * ca - s * sa, s * ca + c * sa) for ca, sa in turns]
            for kind in range(2):
                rows = jnp.concatenate([pair[kind] for pair in pairs], axis=0).astype(jnp.bfloat16)
                table_ref[pl.ds(row_of(kind, a, b), 2 * FINE), lanes] = rows


def dot_last(left, right):
    return lax.dot_general(left, right, (((1,), (1,)), ((), ())), preferred_element_type=jnp.float32)


def filled_product(cos_ref, sin_ref, table_ref, row_of, right_ref, pieces):
    span = table_ref.shape[1] // pieces
    total = None
    for start in range(0, table_ref.shape[1], span):
        for first in range(start, start + span, WIDTH):
            fill_lanes(cos_ref, sin_ref, table_ref, row_of, first)
        lanes = slice(start, start + span)
        piece = dot_last(table_ref[:, lanes], right_ref[:, lanes])
        total = piece if total is None else total + piece
    return total * (1.0 / math.sqrt(table_ref.shape[1]))


def split_parts(x, scale):
    rows, lanes = x.shape
    x = (x * scale).reshape(2, 2, rows // 4, lanes)
    return [x[:, part].reshape(rows // 2, lanes) for part in range(2)]


def forward_kernel(data_ref, cos_ref, sin_ref, spread_ref, table_ref):
    total = filled_product(cos_ref, sin_ref, table_ref, receiver_row, data_ref, 4)
    half = total.shape[0] // 2
    both = jnp.concatenate([total[:half], total[half:]], axis=1)
    spread_ref[...] = both.reshape(spread_ref.shape).astype(jnp.bfloat16)


LEVEL = 13.0
LEAST = 2.0**-100


def turn_kernel(near_ref, turned_ref):
    peers, rows, lanes = near_ref.shape
    shots = lanes // 4
    got = near_ref[...].astype(jnp.float32)
    lines = []
    for kind in range(4):
        pieces = [got[d, :, kind * shots : (kind + 1) * shots] for d in range(peers)]
        lines.append(jnp.concatenate(pieces, axis=1))
    turned = jnp.concatenate(lines, axis=0)
    largest = jnp.maximum(jnp.max(jnp.abs(turned), keepdims=True), LEAST)
    exponent = jnp.ceil(jnp.log2(largest))
    main = 4 * rows
    turned_ref[:main] = (turned * jnp.exp2(LEVEL - exponent)).astype(turned_ref.dtype)
    tail = jnp.broadcast_to(exponent, (turned_ref.shape[0] - main, turned.shape[1]))
    turned_ref[main:] = tail.astype(turned_ref.dtype)


def planes_kernel(far_ref, turned_ref, cos_ref, sin_ref, planes_ref, inner_ref, table_ref, spread_ref):
    peers, _, around = turned_ref.shape
    main = spread_ref.shape[0]
    for far in range(peers):
        block = turned_ref[far].astype(jnp.float32)
        block = block[:main] * jnp.exp2(block[main : main + 1, :1] - LEVEL)
        spread_ref[:, far * around : (far + 1) * around] = block.astype(jnp.bfloat16)
    total = filled_product(cos_ref, sin_ref, table_ref, source_row, spread_ref, 2)
    planes = total.T.astype(jnp.bfloat16)
    planes_ref[...] = planes
    own = table_ref[:, pl.ds(pl.multiple_of(far_ref[0] * around, around), around)]
    total = jnp.dot(planes, own, preferred_element_type=jnp.float32)
    both = jnp.concatenate(split_parts(total, 2.0 / math.sqrt(NSLOW)), axis=1)
    half = both.shape[0] // 2
    inner_ref[:half] = both[:half].astype(jnp.bfloat16)
    inner_ref[half:] = (-both[half:]).astype(jnp.bfloat16)


def back_kernel(planes_ref, inner_ref, back_ref):
    total = jnp.dot(planes_ref[...], inner_ref[...], preferred_element_type=jnp.float32)
    upper, lower = split_parts(total, 2.0 / math.sqrt(NSLOW))
    shots = upper.shape[1] // 2
    real = upper[:, :shots] - lower[:, shots:]
    imaginary = lower[:, :shots] + upper[:, shots:]
    peers, half, lanes = back_ref.shape
    own = lanes // 4
    for peer in range(peers):
        span = slice(peer * own, (peer + 1) * own)
        pieces = [real[:half, span], imaginary[:half, span], real[half:, span], imaginary[half:, span]]
        back_ref[peer] = jnp.concatenate(pieces, axis=1).astype(jnp.bfloat16)


def inverse_kernel(back_ref, cos_ref, sin_ref, out_ref, table_ref):
    peers, half, lanes = back_ref.shape
    turned = back_ref[...].astype(jnp.float32).reshape(peers * half, lanes).T
    back = jnp.concatenate([turned[: lanes // 2], turned[lanes // 2 :]], axis=1).astype(jnp.bfloat16)
    for first in range(0, table_ref.shape[1], WIDTH):
        fill_lanes(cos_ref, sin_ref, table_ref, receiver_row, first)
        lanes = slice(first, first + WIDTH)
        total = jnp.dot(back, table_ref[:, lanes], preferred_element_type=jnp.float32)
        out_ref[:, lanes] = (total * (2.0 / math.sqrt(NSLOW))).astype(jnp.bfloat16)


def call(kernel, shapes, scratch, *operands, dtype=jnp.bfloat16):
    spec = pl.BlockSpec(memory_space=pltpu.VMEM)
    scalar = pl.BlockSpec(memory_space=pltpu.SMEM)
    return pl.pallas_call(
        kernel,
        out_shape=[jax.ShapeDtypeStruct(shape, dtype) for shape in shapes],
        in_specs=[scalar if x.dtype == jnp.int32 else spec for x in operands],
        out_specs=[spec] * len(shapes),
        scratch_shapes=[pltpu.VMEM(shape, jnp.bfloat16) for shape in scratch],
        compiler_params=pltpu.CompilerParams(vmem_limit_bytes=40 * 2**20),
    )(*operands)


def body(recorded, receiver_x, source_x):
    _, _, shots, receivers = recorded.shape
    sources = source_x.shape[0]
    near = ("near", "rep")
    peers = lax.axis_size("near") * lax.axis_size("rep")
    around = peers * shots
    far = lax.axis_index("far").astype(jnp.int32).reshape(1)
    omega = two_pi * (base_hertz + step_hertz * lax.axis_index("freq").astype(jnp.float32))
    data = recorded.reshape(2 * shots, receivers)
    receiver_seeds = seeds(omega, receiver_x)
    receiver_table, source_table = (NSLOW, receivers), (NSLOW, sources)
    columns = 2 * NSLOW // peers
    chunk = (peers, OWNED * FINE * FINE, 4 * shots)

    (spread,) = call(forward_kernel, [chunk], [receiver_table], data, *receiver_seeds)
    spread, source_x = lax.optimization_barrier((spread, source_x))
    spread = lax.all_to_all(spread, near, 0, 0, tiled=True)
    source_seeds = seeds(omega, source_x)
    (turned,) = call(turn_kernel, [(columns + FINE, around)], [], spread, dtype=jnp.float32)
    turned = lax.all_gather(turned.astype(jnp.float16), "far", axis=0, tiled=False).astype(jnp.float32)
    planes, inner = call(
        planes_kernel,
        [(columns, NSLOW), (columns // 2, 2 * around)],
        [source_table, (columns, sources)],
        far,
        turned,
        *source_seeds,
    )
    inner = lax.all_gather(inner, near, axis=0, tiled=True)
    (back,) = call(back_kernel, [chunk], [], planes, inner)
    back = lax.all_to_all(back, near, 0, 0, tiled=True)
    (out,) = call(inverse_kernel, [(2 * shots, receivers)], [receiver_table], back, *receiver_seeds)
    return out.reshape(recorded.shape)


def solution(mesh):
    parts, shot, freq, rep = (mesh.shape[name] for name in ("parts", "shot", "freq", "rep"))
    devices = mesh.devices.reshape(parts, shot // NEAR, NEAR, freq, rep)
    split = Mesh(devices, ("parts", "far", "near", "freq", "rep"))
    placed = P(None, ("parts", "freq"), GROUP, None)
    return jax.shard_map(
        body,
        mesh=split,
        in_specs=(placed, P("parts"), P("parts")),
        out_specs=placed,
        check_vma=False,
    )
```

```python
import math

import jax
import jax.numpy as jnp
from jax import lax
from jax.experimental import pallas as pl
from jax.experimental.pallas import tpu as pltpu
from jax.sharding import Mesh
from jax.sharding import PartitionSpec as P

NSLOW = 1024
FINE = 8
NEAR = 2
OWNED = 2

two_pi = 6.283185307179586
base_hertz = 40.0
step_hertz = 0.5
slow_max = 0.0005

GROUP = ("far", "near", "rep")


def source_row(kind, a, b):
    return (((b // OWNED * 2 + kind) * OWNED + b % OWNED) * FINE + a) * FINE


def receiver_row(kind, a, b):
    return ((kind * FINE + b) * FINE + a) * FINE


def seed_slowness():
    rows = jnp.arange(3 * FINE, dtype=jnp.int32)
    level, index = rows // FINE, rows % FINE
    odd = jnp.where(level == 0, 2 * index + 1, jnp.where(level == 1, 2 * FINE * index, 2 * FINE * FINE * index))
    return slow_max * (odd.astype(jnp.float32) / NSLOW)


def seeds(omega, positions):
    phases = (omega * seed_slowness())[:, None] * positions[None, :]
    return jnp.cos(phases), jnp.sin(phases)


WIDTH = 256


def fill_lanes(cos_ref, sin_ref, table_ref, row_of, first):
    lanes = pl.ds(first, WIDTH)
    c0, s0 = cos_ref[0:FINE, lanes], sin_ref[0:FINE, lanes]
    inner = [(c0, s0)]
    for b in range(1, FINE):
        cb, sb = cos_ref[pl.ds(FINE + b, 1), lanes], sin_ref[pl.ds(FINE + b, 1), lanes]
        inner.append((c0 * cb - s0 * sb, s0 * cb + c0 * sb))
    for a in range(0, FINE, 2):
        turns = [(cos_ref[pl.ds(2 * FINE + k, 1), lanes], sin_ref[pl.ds(2 * FINE + k, 1), lanes]) for k in (a, a + 1)]
        for b, (c, s) in enumerate(inner):
            pairs = [(c * ca - s * sa, s * ca + c * sa) for ca, sa in turns]
            for kind in range(2):
                rows = jnp.concatenate([pair[kind] for pair in pairs], axis=0).astype(jnp.bfloat16)
                table_ref[pl.ds(row_of(kind, a, b), 2 * FINE), lanes] = rows


def dot_last(left, right):
    return lax.dot_general(left, right, (((1,), (1,)), ((), ())), preferred_element_type=jnp.float32)


def filled_product(cos_ref, sin_ref, table_ref, row_of, right_ref, pieces):
    span = table_ref.shape[1] // pieces
    total = None
    for start in range(0, table_ref.shape[1], span):
        for first in range(start, start + span, WIDTH):
            fill_lanes(cos_ref, sin_ref, table_ref, row_of, first)
        lanes = slice(start, start + span)
        piece = dot_last(table_ref[:, lanes], right_ref[:, lanes])
        total = piece if total is None else total + piece
    return total * (1.0 / math.sqrt(table_ref.shape[1]))


def split_parts(x, scale):
    rows, lanes = x.shape
    x = (x * scale).reshape(2, 2, rows // 4, lanes)
    return [x[:, part].reshape(rows // 2, lanes) for part in range(2)]


def forward_kernel(data_ref, cos_ref, sin_ref, spread_ref, table_ref):
    total = filled_product(cos_ref, sin_ref, table_ref, receiver_row, data_ref, 4)
    half = total.shape[0] // 2
    both = jnp.concatenate([total[:half], total[half:]], axis=1)
    spread_ref[...] = both.reshape(spread_ref.shape).astype(jnp.bfloat16)


LEVEL = 13.0
LEAST = 2.0**-100


def turn_kernel(near_ref, turned_ref):
    peers, rows, lanes = near_ref.shape
    shots = lanes // 4
    got = near_ref[...].astype(jnp.float32)
    lines = []
    for kind in range(4):
        pieces = [got[d, :, kind * shots : (kind + 1) * shots] for d in range(peers)]
        lines.append(jnp.concatenate(pieces, axis=1))
    turned = jnp.concatenate(lines, axis=0)
    largest = jnp.maximum(jnp.max(jnp.abs(turned), keepdims=True), LEAST)
    exponent = jnp.ceil(jnp.log2(largest))
    main = 4 * rows
    turned_ref[:main] = (turned * jnp.exp2(LEVEL - exponent)).astype(turned_ref.dtype)
    tail = jnp.broadcast_to(exponent, (turned_ref.shape[0] - main, turned.shape[1]))
    turned_ref[main:] = tail.astype(turned_ref.dtype)


def planes_kernel(far_ref, turned_ref, cos_ref, sin_ref, planes_ref, inner_ref, table_ref, spread_ref):
    peers, _, around = turned_ref.shape
    main = spread_ref.shape[0]
    for far in range(peers):
        block = turned_ref[far].astype(jnp.float32)
        block = block[:main] * jnp.exp2(block[main : main + 1, :1] - LEVEL)
        spread_ref[:, far * around : (far + 1) * around] = block.astype(jnp.bfloat16)
    total = filled_product(cos_ref, sin_ref, table_ref, source_row, spread_ref, 2)
    planes = total.T.astype(jnp.bfloat16)
    planes_ref[...] = planes
    own = table_ref[:, pl.ds(pl.multiple_of(far_ref[0] * around, around), around)]
    total = jnp.dot(planes, own, preferred_element_type=jnp.float32)
    both = jnp.concatenate(split_parts(total, 2.0 / math.sqrt(NSLOW)), axis=1)
    half = both.shape[0] // 2
    inner_ref[:half] = both[:half].astype(jnp.bfloat16)
    inner_ref[half:] = (-both[half:]).astype(jnp.bfloat16)


def back_kernel(planes_ref, inner_ref, back_ref):
    total = jnp.dot(planes_ref[...], inner_ref[...], preferred_element_type=jnp.float32)
    upper, lower = split_parts(total, 2.0 / math.sqrt(NSLOW))
    shots = upper.shape[1] // 2
    real = upper[:, :shots] - lower[:, shots:]
    imaginary = lower[:, :shots] + upper[:, shots:]
    peers, half, lanes = back_ref.shape
    own = lanes // 4
    for peer in range(peers):
        span = slice(peer * own, (peer + 1) * own)
        pieces = [real[:half, span], imaginary[:half, span], real[half:, span], imaginary[half:, span]]
        back_ref[peer] = jnp.concatenate(pieces, axis=1).astype(jnp.bfloat16)


def inverse_kernel(back_ref, cos_ref, sin_ref, out_ref, table_ref):
    peers, half, lanes = back_ref.shape
    turned = back_ref[...].astype(jnp.float32).reshape(peers * half, lanes).T
    back = jnp.concatenate([turned[: lanes // 2], turned[lanes // 2 :]], axis=1).astype(jnp.bfloat16)
    for first in range(0, table_ref.shape[1], WIDTH):
        fill_lanes(cos_ref, sin_ref, table_ref, receiver_row, first)
        lanes = slice(first, first + WIDTH)
        total = jnp.dot(back, table_ref[:, lanes], preferred_element_type=jnp.float32)
        out_ref[:, lanes] = (total * (2.0 / math.sqrt(NSLOW))).astype(jnp.bfloat16)


def call(kernel, shapes, scratch, *operands, dtype=jnp.bfloat16):
    spec = pl.BlockSpec(memory_space=pltpu.VMEM)
    scalar = pl.BlockSpec(memory_space=pltpu.SMEM)
    return pl.pallas_call(
        kernel,
        out_shape=[jax.ShapeDtypeStruct(shape, dtype) for shape in shapes],
        in_specs=[scalar if x.dtype == jnp.int32 else spec for x in operands],
        out_specs=[spec] * len(shapes),
        scratch_shapes=[pltpu.VMEM(shape, jnp.bfloat16) for shape in scratch],
        compiler_params=pltpu.CompilerParams(vmem_limit_bytes=40 * 2**20),
    )(*operands)


def body(recorded, receiver_x, source_x):
    _, _, shots, receivers = recorded.shape
    sources = source_x.shape[0]
    near = ("near", "rep")
    peers = lax.axis_size("near") * lax.axis_size("rep")
    around = peers * shots
    far = lax.axis_index("far").astype(jnp.int32).reshape(1)
    omega = two_pi * (base_hertz + step_hertz * lax.axis_index("freq").astype(jnp.float32))
    data = recorded.reshape(2 * shots, receivers)
    receiver_seeds = seeds(omega, receiver_x)
    receiver_table, source_table = (NSLOW, receivers), (NSLOW, sources)
    columns = 2 * NSLOW // peers
    chunk = (peers, OWNED * FINE * FINE, 4 * shots)

    (spread,) = call(forward_kernel, [chunk], [receiver_table], data, *receiver_seeds)
    spread, source_x = lax.optimization_barrier((spread, source_x))
    spread = lax.all_to_all(spread, near, 0, 0, tiled=True)
    source_seeds = seeds(omega, source_x)
    (turned,) = call(turn_kernel, [(columns + FINE, around)], [], spread, dtype=jnp.float32)
    block = turned.shape
    turned = lax.all_gather(turned.astype(jnp.float16).reshape(-1), "far", axis=0, tiled=True)
    turned = turned.reshape(-1, *block).astype(jnp.float32)
    planes, inner = call(
        planes_kernel,
        [(columns, NSLOW), (columns // 2, 2 * around)],
        [source_table, (columns, sources)],
        far,
        turned,
        *source_seeds,
    )
    inner = lax.all_gather(inner, near, axis=0, tiled=True)
    (back,) = call(back_kernel, [chunk], [], planes, inner)
    back = lax.all_to_all(back, near, 0, 0, tiled=True)
    (out,) = call(inverse_kernel, [(2 * shots, receivers)], [receiver_table], back, *receiver_seeds)
    return out.reshape(recorded.shape)


def solution(mesh):
    parts, shot, freq, rep = (mesh.shape[name] for name in ("parts", "shot", "freq", "rep"))
    devices = mesh.devices.reshape(parts, shot // NEAR, NEAR, freq, rep)
    split = Mesh(devices, ("parts", "far", "near", "freq", "rep"))
    placed = P(None, ("parts", "freq"), GROUP, None)
    return jax.shard_map(
        body,
        mesh=split,
        in_specs=(placed, P("parts"), P("parts")),
        out_specs=placed,
        check_vma=False,
    )
```
